256 devices in a mesh: outer: 16 (over z_lo, x), inner: 16 (over y, z_hi, core).
Axes of the slice: x: 4, y: 4, z: 8 (z_hi: 2, z_lo: 4; z = z_hi * 4 + z_lo), core: 2. Of those that a mesh axis runs over, the one named last changes fastest.
Arguments:
- queries: bfloat16 [8192, 2, 4096], P('outer', None, 'inner'), may hold values from -52 to 52
- keys: bfloat16 [8192, 2, 4096], P('outer', None, 'inner'), may hold values from -6 to 6
- values: bfloat16 [8192, 2, 4096], P('outer', None, 'inner'), may hold values from -6 to 6
Outputs:
- attended: bfloat16 [8192, 2, 4096], P(('outer', 'inner'))
The draws below stay inside these ranges and needn't reach their ends.
All inputs are finite; a program needn't handle non-finite values.
Results may differ from the reference program's by a relative error of at most 0.004.
Values may be sent and summed in bfloat16 or wider, within the bound.
No kernel may reach another device: no remote copies, remote signals or barrier semaphores. Data moves between devices by JAX's collectives and lax.ppermute only.
A program may use at most 128 MiB of HBM per device.

```python
import math
import jax
import jax.numpy as jnp
from jax import lax

NETWORKS = 2
HEADS = 32
HEAD_DIM = 128
WIDTH = 4096
SEQ = 8192


def key_field(key):
    base = jax.random.fold_in(key, 11)
    field = jnp.clip(jax.random.normal(base, (SEQ, NETWORKS, WIDTH), jnp.float32), -6.0, 6.0)
    return field


def draw_keys(key, part):
    return key_field(key).astype(jnp.bfloat16)


def draw_queries(key, part):
    base = jax.random.fold_in(key, 12)
    result = 3.0 * jnp.clip(jax.random.normal(base, (SEQ, NETWORKS, WIDTH), jnp.float32), -6.0, 6.0)
    return result.astype(jnp.bfloat16)


def steps_of(rng, shape, shards, low, high):
    factor_of, own = 1.0, jax.random.fold_in(rng, 6)
    for axis_at, shards_of in shards:
        draws = jnp.exp(jax.random.uniform(jax.random.fold_in(own, axis_at), (shards_of,), jnp.float32, low / len(shards), high / len(shards)))
        factor_of = factor_of * jnp.repeat(draws, shape[axis_at] // shards_of).reshape([-1 if axis == axis_at else 1 for axis in range(len(shape))])
    return factor_of


def scatter_about(rng, extent, scale, reach, pieces=(), kind=jnp.bfloat16):
    gain = steps_of(rng, extent, pieces, -0.22, 0.18) if pieces else 1.0
    values = jax.random.normal(rng, extent, jnp.float32) * scale * gain
    return jnp.minimum(jnp.maximum(values, -reach), reach).astype(kind)


def setup_inputs(seed: int = 0) -> dict:
    splits = jax.random.split(jax.random.key(seed), 4)
    queries = draw_queries(jax.random.fold_in(splits[3], 71), 0)
    keys = draw_keys(jax.random.fold_in(splits[3], 71), 0)
    values = scatter_about(splits[2], (SEQ, NETWORKS, WIDTH), 1.0, 6.0, ((0, 16), (2, 16)))
    return dict(queries=queries, keys=keys, values=values)


def attend_rows(query_rows, key_rows, value_rows):
    scores = jnp.dot(query_rows, key_rows.T, preferred_element_type=jnp.float32) * (1.0 / math.sqrt(HEAD_DIM))
    peak_rows = lax.optimization_barrier(jnp.max(scores, axis=1, keepdims=True))
    weights = jnp.exp(scores - peak_rows)
    totals = lax.optimization_barrier(jnp.sum(weights, axis=1, keepdims=True))
    numerator = jnp.dot(weights.astype(jnp.bfloat16), value_rows, preferred_element_type=jnp.float32)
    return numerator / totals

def attend_pair(inputs):
    query_rows, key_rows, value_rows = inputs
    blocks = query_rows.reshape(16, SEQ // 16, HEAD_DIM)
    result = lax.map(lambda block: attend_rows(block, key_rows, value_rows), blocks)
    return result.reshape(SEQ, HEAD_DIM)

def split_heads(array):
    return array.reshape(SEQ, NETWORKS, HEADS, HEAD_DIM).transpose(1, 2, 0, 3).reshape(NETWORKS * HEADS, SEQ, HEAD_DIM)

def reference(queries, keys, values):
    averaged = lax.map(attend_pair, (split_heads(queries), split_heads(keys), split_heads(values)))
    averaged = averaged.reshape(NETWORKS, HEADS, SEQ, HEAD_DIM).transpose(2, 0, 1, 3)
    return averaged.reshape(SEQ, NETWORKS, WIDTH).astype(jnp.bfloat16)
```

```python
from functools import partial
import math

import jax
import jax.numpy as jnp
from jax import lax
from jax.experimental import pallas as pl
from jax.experimental.pallas import tpu as pltpu
from jax.sharding import Mesh, PartitionSpec as P


HEAD_DIM = 128
LOG2_SCALE = math.log2(math.e) / math.sqrt(HEAD_DIM)
SUM_ROWS = 16
PIECE = 256
Q_TILE = 512
VMEM_BYTES = 24 * 1024 * 1024


def pack_kernel(zl_ref, q_ref, k_ref, v_ref, *out_refs):
    for s in range(4):
        q_out, c0_out, c1_out = out_refs[3 * s:3 * s + 3]
        at = pl.multiple_of(lax.rem(zl_ref[0] + s, 4) * HEAD_DIM, HEAD_DIM)
        head = pl.ds(at, HEAD_DIM)
        q_out[...] = q_ref[:, head]
        c0_out[0] = k_ref[0:PIECE, head]
        c0_out[1] = v_ref[0:PIECE, head]
        c1_out[0] = k_ref[PIECE:, head]
        c1_out[1] = v_ref[PIECE:, head]


def pack_heads(zl, queries, keys, values):
    rows = queries.shape[0]
    flat = [a.reshape(rows, 4 * HEAD_DIM) for a in (queries, keys, values)]
    vmem = pl.BlockSpec(memory_space=pltpu.VMEM)
    kv_shape = jax.ShapeDtypeStruct((2, PIECE, HEAD_DIM), jnp.bfloat16)
    q_shape = jax.ShapeDtypeStruct((rows, HEAD_DIM), jnp.bfloat16)
    outs = pl.pallas_call(
        pack_kernel,
        in_specs=[pl.BlockSpec(memory_space=pltpu.SMEM), vmem, vmem, vmem],
        out_specs=[vmem] * 12,
        out_shape=[q_shape, kv_shape, kv_shape] * 4,
        compiler_params=pltpu.CompilerParams(vmem_limit_bytes=VMEM_BYTES),
        name="pack",
    )(zl, *flat)
    return outs[0::3], outs[1::3], outs[2::3]


def flash_kernel(first, last, counts, zl_ref, q_ref, *refs):
    kv_refs, refs = refs[: len(counts)], refs[len(counts):]
    if not first:
        peak_in, acc_in, *refs = refs
    if last:
        out_ref, vt_ref = refs
    else:
        peak_out, acc_out, vt_ref = refs
    pieces = [(ref, p) for ref, count in zip(kv_refs, counts) for p in range(count)]

    @pl.when(pl.program_id(0) == 0)
    def _():
        for at, (ref, p) in enumerate(pieces):
            vt_ref[0:HEAD_DIM, at * PIECE:(at + 1) * PIECE] = ref[p, 1].T
        vt_ref[HEAD_DIM:, :] = jnp.ones((SUM_ROWS, vt_ref.shape[1]), jnp.bfloat16)

    queries = q_ref[0]
    tile = queries.shape[0]
    if first:
        peak = jnp.full((1, tile), -1e30, jnp.float32)
        acc = jnp.zeros((HEAD_DIM + SUM_ROWS, tile), jnp.float32)
    else:
        peak = peak_in[0:1, :]
        acc = acc_in[...]

    def score(at):
        keys = jnp.concatenate([ref[p, 0] for ref, p in pieces[at:at + 2]], axis=0)
        return lax.dot_general(
            keys, queries, (((1,), (1,)), ((), ())), preferred_element_type=jnp.float32
        )

    scores = score(0)
    for at in range(0, len(pieces), 2):
        following = score(at + 2) if at + 2 < len(pieces) else None
        new_peak = jnp.maximum(peak, jnp.max(scores, axis=0, keepdims=True))
        shift = new_peak * LOG2_SCALE
        weights = jnp.exp2(scores * LOG2_SCALE - shift).astype(jnp.bfloat16)
        shrink = jnp.exp2(peak * LOG2_SCALE - shift)
        acc = acc * shrink + jnp.dot(
            vt_ref[:, at * PIECE:(at + 2) * PIECE], weights, preferred_element_type=jnp.float32
        )
        peak, scores = new_peak, following
    if last:
        attended = acc[0:HEAD_DIM, :] / acc[HEAD_DIM:HEAD_DIM + 1, :]
        out_ref[0] = attended.T.astype(jnp.bfloat16)
    else:
        peak_out[...] = jnp.broadcast_to(peak, peak_out.shape)
        acc_out[...] = acc


def flash(zl, queries, blocks, state, last):
    sources, rows, _ = queries.shape
    per_source = rows // Q_TILE
    total = sources * rows
    counts = tuple(b.shape[0] for b in blocks)
    first = state is None
    q_spec = pl.BlockSpec((1, Q_TILE, HEAD_DIM), lambda i, z: (i // per_source, i % per_source, 0))
    in_specs = [q_spec] + [
        pl.BlockSpec((c, 2, PIECE, HEAD_DIM), lambda i, z: (0, 0, 0, 0)) for c in counts
    ]
    peak_spec = pl.BlockSpec((8, Q_TILE), lambda i, z: (0, i))
    acc_spec = pl.BlockSpec((HEAD_DIM + SUM_ROWS, Q_TILE), lambda i, z: (0, i))
    args = [queries, *blocks]
    if not first:
        in_specs += [peak_spec, acc_spec]
        args += list(state)
    if last:
        out_specs = pl.BlockSpec(
            (1, Q_TILE, HEAD_DIM),
            lambda i, z: (lax.rem(z[0] + 4 - i // per_source, 4), i % per_source, 0),
        )
        out_shape = jax.ShapeDtypeStruct(queries.shape, jnp.bfloat16)
    else:
        out_specs = [peak_spec, acc_spec]
        out_shape = [
            jax.ShapeDtypeStruct((8, total), jnp.float32),
            jax.ShapeDtypeStruct((HEAD_DIM + SUM_ROWS, total), jnp.float32),
        ]
    key_count = sum(counts) * PIECE
    return pl.pallas_call(
        partial(flash_kernel, first, last, counts),
        grid_spec=pltpu.PrefetchScalarGridSpec(
            num_scalar_prefetch=1,
            grid=(total // Q_TILE,),
            in_specs=in_specs,
            out_specs=out_specs,
            scratch_shapes=[pltpu.VMEM((HEAD_DIM + SUM_ROWS, key_count), jnp.bfloat16)],
        ),
        out_shape=out_shape,
        compiler_params=pltpu.CompilerParams(
            dimension_semantics=("arbitrary",), vmem_limit_bytes=VMEM_BYTES
        ),
        cost_estimate=pl.CostEstimate(
            flops=16 * total * key_count * HEAD_DIM,
            bytes_accessed=2 * (total + 2 * key_count) * HEAD_DIM,
            transcendentals=total * key_count,
        ),
        name="flash",
    )(zl, *args)


def shift(array, axis, by):
    return lax.ppermute(array, axis, [(i, (i + by) % 4) for i in range(4)])


def to_heads(packed):
    parts = [packed[0]]
    for s in (1, 2, 3):
        parts.append(shift(packed[s], "zl", s))
    return jnp.stack(parts)


def around_ring(block):
    left = shift(block, "x", 1)
    right = shift(block, "x", -1)
    half = block.shape[0] // 2
    far_a = shift(left[:half], "x", 1)
    far_b = shift(right[half:], "x", -1)
    return left, right, [far_a, far_b]


def attention(queries, keys, values):
    rows = queries.shape[0]
    zl = lax.axis_index("zl").astype(jnp.int32).reshape(1)
    q_packed, c0, c1 = pack_heads(zl, queries, keys, values)
    own0 = to_heads(c0)
    q_all = to_heads(q_packed)
    own1 = to_heads(c1)
    left0, right0, far0 = around_ring(own0)
    left1, right1, far1 = around_ring(own1)
    steps = [
        ("own0", [own0]), ("left0", [left0]), ("right0", [right0]), ("far0", far0),
        ("own1", [own1]), ("near1", [left1, right1]), ("far1", far1),
    ]
    state = None
    for name, blocks in steps:
        state = flash(zl, q_all, blocks, state, name == "far1")
    blocks = state.reshape(64, rows // 16, HEAD_DIM)
    blocks = lax.all_to_all(blocks, ("zl", "y", "zh", "c"), 0, 0, tiled=True)
    out = blocks.reshape(2, 2, 16, rows // 16, HEAD_DIM).transpose(3, 0, 2, 1, 4)
    return out.reshape(rows // 16, 2, 32 * HEAD_DIM)


def solution(mesh):
    grid = Mesh(mesh.devices.reshape(4, 4, 4, 2, 2), ("zl", "x", "y", "zh", "c"))
    spec = P(("zl", "x"), None, ("y", "zh", "c"))
    return jax.shard_map(
        attention,
        mesh=grid,
        in_specs=(spec, spec, spec),
        out_specs=P(("zl", "x", "y", "zh", "c"), None, None),
        check_vma=False,
    )
```

```python
from functools import partial
import math

import jax
import jax.numpy as jnp
from jax import lax
from jax.experimental import pallas as pl
from jax.experimental.pallas import tpu as pltpu
from jax.sharding import Mesh, PartitionSpec as P


HEAD_DIM = 128
LOG2_SCALE = math.log2(math.e) / math.sqrt(HEAD_DIM)
SUM_ROWS = 16
PIECE = 256
Q_TILE = 512
VMEM_BYTES = 24 * 1024 * 1024


def pack_kernel(zl_ref, q_ref, k_ref, v_ref, *out_refs):
    for s in range(4):
        q_out, c0_out, c1_out = out_refs[3 * s:3 * s + 3]
        at = pl.multiple_of((zl_ref[0] ^ s) * HEAD_DIM, HEAD_DIM)
        head = pl.ds(at, HEAD_DIM)
        q_out[...] = q_ref[:, head]
        c0_out[0] = k_ref[0:PIECE, head]
        c0_out[1] = v_ref[0:PIECE, head]
        c1_out[0] = k_ref[PIECE:, head]
        c1_out[1] = v_ref[PIECE:, head]


def pack_heads(zl, queries, keys, values):
    rows = queries.shape[0]
    flat = [a.reshape(rows, 4 * HEAD_DIM) for a in (queries, keys, values)]
    vmem = pl.BlockSpec(memory_space=pltpu.VMEM)
    kv_shape = jax.ShapeDtypeStruct((2, PIECE, HEAD_DIM), jnp.bfloat16)
    q_shape = jax.ShapeDtypeStruct((rows, HEAD_DIM), jnp.bfloat16)
    outs = pl.pallas_call(
        pack_kernel,
        in_specs=[pl.BlockSpec(memory_space=pltpu.SMEM), vmem, vmem, vmem],
        out_specs=[vmem] * 12,
        out_shape=[q_shape, kv_shape, kv_shape] * 4,
        compiler_params=pltpu.CompilerParams(vmem_limit_bytes=VMEM_BYTES),
        name="pack",
    )(zl, *flat)
    return outs[0::3], outs[1::3], outs[2::3]


def flash_kernel(first, last, counts, at_ref, q_ref, *refs):
    kv_refs, refs = refs[: len(counts)], refs[len(counts):]
    if not first:
        peak_in, acc_in, *refs = refs
    if last:
        out_ref, vt_ref = refs
    else:
        peak_out, acc_out, vt_ref = refs
    pieces = [(ref, p) for ref, count in zip(kv_refs, counts) for p in range(count)]

    @pl.when(pl.program_id(0) == 0)
    def _():
        for at, (ref, p) in enumerate(pieces):
            vt_ref[0:HEAD_DIM, at * PIECE:(at + 1) * PIECE] = ref[p, 1].T
        vt_ref[HEAD_DIM:, :] = jnp.ones((SUM_ROWS, vt_ref.shape[1]), jnp.bfloat16)

    queries = q_ref[0]
    tile = queries.shape[0]
    if first:
        peak = jnp.full((1, tile), -1e30, jnp.float32)
        acc = jnp.zeros((HEAD_DIM + SUM_ROWS, tile), jnp.float32)
    else:
        peak = peak_in[0:1, :]
        acc = acc_in[...]

    def score(at):
        keys = jnp.concatenate([ref[p, 0] for ref, p in pieces[at:at + 2]], axis=0)
        return lax.dot_general(
            keys, queries, (((1,), (1,)), ((), ())), preferred_element_type=jnp.float32
        )

    scores = score(0)
    for at in range(0, len(pieces), 2):
        following = score(at + 2) if at + 2 < len(pieces) else None
        new_peak = jnp.maximum(peak, jnp.max(scores, axis=0, keepdims=True))
        shift = new_peak * LOG2_SCALE
        weights = jnp.exp2(scores * LOG2_SCALE - shift).astype(jnp.bfloat16)
        shrink = jnp.exp2(peak * LOG2_SCALE - shift)
        acc = acc * shrink + jnp.dot(
            vt_ref[:, at * PIECE:(at + 2) * PIECE], weights, preferred_element_type=jnp.float32
        )
        peak, scores = new_peak, following
    if last:
        attended = acc[0:HEAD_DIM, :] / acc[HEAD_DIM:HEAD_DIM + 1, :]
        rows = attended.T.astype(jnp.bfloat16).reshape(8, 2, tile // 16, HEAD_DIM)
        for core in range(2):
            out_ref[0, :, core ^ at_ref[1]] = rows[:, core]
    else:
        peak_out[...] = jnp.broadcast_to(peak, peak_out.shape)
        acc_out[...] = acc


def flash(at, queries, blocks, state, last):
    tiles = queries.shape[0]
    counts = tuple(b.shape[0] for b in blocks)
    first = state is None
    q_spec = pl.BlockSpec((1, Q_TILE, HEAD_DIM), lambda i, at: (i, 0, 0))
    in_specs = [q_spec] + [
        pl.BlockSpec((c, 2, PIECE, HEAD_DIM), lambda i, at: (0, 0, 0, 0)) for c in counts
    ]
    peak_spec = pl.BlockSpec((8, Q_TILE), lambda i, at: (0, i))
    acc_spec = pl.BlockSpec((HEAD_DIM + SUM_ROWS, Q_TILE), lambda i, at: (0, i))
    args = [queries, *blocks]
    if not first:
        in_specs += [peak_spec, acc_spec]
        args += list(state)
    if last:
        strip = Q_TILE // 16
        out_specs = pl.BlockSpec(
            (1, 8, 2, strip, HEAD_DIM), lambda i, at: (at[0] ^ i, 0, 0, 0, 0)
        )
        out_shape = jax.ShapeDtypeStruct((tiles, 8, 2, strip, HEAD_DIM), jnp.bfloat16)
    else:
        out_specs = [peak_spec, acc_spec]
        out_shape = [
            jax.ShapeDtypeStruct((8, tiles * Q_TILE), jnp.float32),
            jax.ShapeDtypeStruct((HEAD_DIM + SUM_ROWS, tiles * Q_TILE), jnp.float32),
        ]
    key_count = sum(counts) * PIECE
    total = tiles * Q_TILE
    return pl.pallas_call(
        partial(flash_kernel, first, last, counts),
        grid_spec=pltpu.PrefetchScalarGridSpec(
            num_scalar_prefetch=1,
            grid=(tiles,),
            in_specs=in_specs,
            out_specs=out_specs,
            scratch_shapes=[pltpu.VMEM((HEAD_DIM + SUM_ROWS, key_count), jnp.bfloat16)],
        ),
        out_shape=out_shape,
        compiler_params=pltpu.CompilerParams(
            dimension_semantics=("arbitrary",), vmem_limit_bytes=VMEM_BYTES
        ),
        cost_estimate=pl.CostEstimate(
            flops=16 * total * key_count * HEAD_DIM,
            bytes_accessed=2 * (total + 2 * key_count) * HEAD_DIM,
            transcendentals=total * key_count,
        ),
        name="flash",
    )(at, *args)


def gate_kernel(in_ref, out_ref):
    out_ref[0] = in_ref[0]
    out_ref[1] = in_ref[1]


def gate(position):
    return pl.pallas_call(
        gate_kernel,
        in_specs=[pl.BlockSpec(memory_space=pltpu.SMEM)],
        out_specs=pl.BlockSpec(memory_space=pltpu.SMEM),
        out_shape=jax.ShapeDtypeStruct((2,), jnp.int32),
        compiler_params=pltpu.CompilerParams(vmem_limit_bytes=VMEM_BYTES),
        name="gate",
    )(position)


def shift(array, by):
    return lax.ppermute(array, "x", [(i, (i + by) % 4) for i in range(4)])


def to_heads(packed):
    parts = [packed[0]]
    for s in (1, 2, 3):
        parts.append(lax.ppermute(packed[s], "zl", [(i, i ^ s) for i in range(4)]))
    return jnp.stack(parts)


def neighbours(block):
    left = shift(block, 1)
    right = shift(block, -1)
    return [left, right]


def forwarded(near0, near1):
    half = near0[0].shape[0] // 2
    far_a = shift(jnp.concatenate([near0[0][:half], near1[0][:half]]), 1)
    far_b = shift(jnp.concatenate([near0[1][half:], near1[1][half:]]), -1)
    return [far_a, far_b]


def attention(queries, keys, values):
    rows = queries.shape[0]
    position = jnp.stack([lax.axis_index("zl"), lax.axis_index("c")]).astype(jnp.int32)
    q_packed, c0, c1 = pack_heads(position, queries, keys, values)
    own0 = to_heads(c0)
    own1 = to_heads(c1)
    q_all = to_heads(q_packed)
    near0 = neighbours(own0)
    near1 = neighbours(own1)
    far = forwarded(near0, near1)
    state = None
    at = gate(position)
    for name, blocks in (("1", [own0, *near0]), ("2", [own1, *near1]), ("3", far)):
        state = flash(at, q_all, blocks, state, name == "3")
    return to_tokens(state, rows // 16)


def to_tokens(attended, strip):
    blocks = attended.reshape(32, 2 * strip, HEAD_DIM)
    blocks = lax.all_to_all(blocks, ("zl", "y", "zh"), 0, 0, tiled=True)
    blocks = blocks.reshape(32, 2, strip, HEAD_DIM)
    own = blocks[:, 0]
    other = lax.ppermute(blocks[:, 1], "c", [(0, 1), (1, 0)])
    first = lax.axis_index("c") == 0
    both = jnp.stack([jnp.where(first, own, other), jnp.where(first, other, own)], axis=1)
    out = both.reshape(2, 2, 16, strip, HEAD_DIM).transpose(3, 0, 2, 1, 4)
    return out.reshape(strip, 2, 32 * HEAD_DIM)


def solution(mesh):
    grid = Mesh(mesh.devices.reshape(4, 4, 4, 2, 2), ("zl", "x", "y", "zh", "c"))
    spec = P(("zl", "x"), None, ("y", "zh", "c"))
    return jax.shard_map(
        attention,
        mesh=grid,
        in_specs=(spec, spec, spec),
        out_specs=P(("zl", "x", "y", "zh", "c"), None, None),
        check_vma=False,
    )
```

```python
from functools import partial
import math

import jax
import jax.numpy as jnp
from jax import lax
from jax.experimental import pallas as pl
from jax.experimental.pallas import tpu as pltpu
from jax.sharding import Mesh, PartitionSpec as P


HEAD_DIM = 128
LOG2_SCALE = math.log2(math.e) / math.sqrt(HEAD_DIM)
SUM_ROWS = 16
PIECE = 256
Q_TILE = 512
MAX_STEP = 6
VMEM_BYTES = 24 * 1024 * 1024


def pack_kv_kernel(start, at_ref, k_ref, v_ref, *out_refs):
    for s in range(4):
        head = pl.ds(pl.multiple_of((at_ref[0] ^ s) * HEAD_DIM, HEAD_DIM), HEAD_DIM)
        out_refs[s][0] = k_ref[start:start + PIECE, head]
        out_refs[s][1] = v_ref[start:start + PIECE, head]


def pack_q_kernel(at_ref, q_ref, *out_refs):
    for s in range(4):
        head = pl.ds(pl.multiple_of((at_ref[0] ^ s) * HEAD_DIM, HEAD_DIM), HEAD_DIM)
        out_refs[s][...] = q_ref[:, head]


def pack(kernel, position, arrays, shapes):
    rows = arrays[0].shape[0]
    flat = [a.reshape(rows, 4 * HEAD_DIM) for a in arrays]
    vmem = pl.BlockSpec(memory_space=pltpu.VMEM)
    return pl.pallas_call(
        kernel,
        in_specs=[pl.BlockSpec(memory_space=pltpu.SMEM)] + [vmem] * len(flat),
        out_specs=[vmem] * (4 * len(shapes)),
        out_shape=[jax.ShapeDtypeStruct(shape, jnp.bfloat16) for shape in shapes] * 4,
        compiler_params=pltpu.CompilerParams(vmem_limit_bytes=VMEM_BYTES),
    )(position, *flat)


def flash_kernel(first, last, counts, at_ref, q_ref, *refs):
    kv_refs, refs = refs[: len(counts)], refs[len(counts):]
    if not first:
        peak_in, acc_in, *refs = refs
    if last:
        out_ref, vt_ref = refs
    else:
        peak_out, acc_out, vt_ref = refs
    pieces = [(ref, p) for ref, count in zip(kv_refs, counts) for p in range(count)]

    @pl.when(pl.program_id(0) == 0)
    def _():
        for at, (ref, p) in enumerate(pieces):
            vt_ref[0:HEAD_DIM, at * PIECE:(at + 1) * PIECE] = ref[p, 1].T
        vt_ref[HEAD_DIM:, :] = jnp.ones((SUM_ROWS, vt_ref.shape[1]), jnp.bfloat16)

    queries = q_ref[0]
    tile = queries.shape[0]
    if first:
        peak = jnp.full((1, tile), -1e30, jnp.float32)
        acc = jnp.zeros((HEAD_DIM + SUM_ROWS, tile), jnp.float32)
    else:
        peak = peak_in[0:1, :]
        acc = acc_in[...]

    step = -(-len(pieces) // -(-len(pieces) // MAX_STEP))

    def score(at):
        keys = jnp.concatenate([ref[p, 0] for ref, p in pieces[at:at + step]], axis=0)
        return lax.dot_general(
            keys, queries, (((1,), (1,)), ((), ())), preferred_element_type=jnp.float32
        )

    scores = score(0)
    for at in range(0, len(pieces), step):
        following = score(at + step) if at + step < len(pieces) else None
        new_peak = jnp.maximum(peak, jnp.max(scores, axis=0, keepdims=True))
        shift = new_peak * LOG2_SCALE
        weights = jnp.exp2(scores * LOG2_SCALE - shift).astype(jnp.bfloat16)
        shrink = jnp.exp2(peak * LOG2_SCALE - shift)
        acc = acc * shrink + jnp.dot(
            vt_ref[:, at * PIECE:min(at + step, len(pieces)) * PIECE], weights, preferred_element_type=jnp.float32
        )
        peak, scores = new_peak, following
    if last:
        attended = acc[0:HEAD_DIM, :] / acc[HEAD_DIM:HEAD_DIM + 1, :]
        rows = attended.T.astype(jnp.bfloat16).reshape(8, 2, tile // 16, HEAD_DIM)
        for core in range(2):
            out_ref[0, :, core ^ at_ref[1]] = rows[:, core]
    else:
        peak_out[...] = jnp.broadcast_to(peak, peak_out.shape)
        acc_out[...] = acc


def flash(at, queries, blocks, state, last):
    tiles = queries.shape[0]
    counts = tuple(b.shape[0] for b in blocks)
    first = state is None
    q_spec = pl.BlockSpec((1, Q_TILE, HEAD_DIM), lambda i, at: (i, 0, 0))
    in_specs = [q_spec] + [
        pl.BlockSpec((c, 2, PIECE, HEAD_DIM), lambda i, at: (0, 0, 0, 0)) for c in counts
    ]
    peak_spec = pl.BlockSpec((8, Q_TILE), lambda i, at: (0, i))
    acc_spec = pl.BlockSpec((HEAD_DIM + SUM_ROWS, Q_TILE), lambda i, at: (0, i))
    args = [queries, *blocks]
    if not first:
        in_specs += [peak_spec, acc_spec]
        args += list(state)
    if last:
        strip = Q_TILE // 16
        out_specs = pl.BlockSpec(
            (1, 8, 2, strip, HEAD_DIM), lambda i, at: (at[0] ^ i, 0, 0, 0, 0)
        )
        out_shape = jax.ShapeDtypeStruct((tiles, 8, 2, strip, HEAD_DIM), jnp.bfloat16)
    else:
        out_specs = [peak_spec, acc_spec]
        out_shape = [
            jax.ShapeDtypeStruct((8, tiles * Q_TILE), jnp.float32),
            jax.ShapeDtypeStruct((HEAD_DIM + SUM_ROWS, tiles * Q_TILE), jnp.float32),
        ]
    key_count = sum(counts) * PIECE
    total = tiles * Q_TILE
    return pl.pallas_call(
        partial(flash_kernel, first, last, counts),
        grid_spec=pltpu.PrefetchScalarGridSpec(
            num_scalar_prefetch=1,
            grid=(tiles,),
            in_specs=in_specs,
            out_specs=out_specs,
            scratch_shapes=[pltpu.VMEM((HEAD_DIM + SUM_ROWS, key_count), jnp.bfloat16)],
        ),
        out_shape=out_shape,
        compiler_params=pltpu.CompilerParams(
            dimension_semantics=("arbitrary",), vmem_limit_bytes=VMEM_BYTES
        ),
        cost_estimate=pl.CostEstimate(
            flops=16 * total * key_count * HEAD_DIM,
            bytes_accessed=2 * (total + 2 * key_count) * HEAD_DIM,
            transcendentals=total * key_count,
        ),
        name="flash",
    )(at, *args)


def gate_kernel(in_ref, out_ref):
    out_ref[0] = in_ref[0]
    out_ref[1] = in_ref[1]


def gate(position):
    return pl.pallas_call(
        gate_kernel,
        in_specs=[pl.BlockSpec(memory_space=pltpu.SMEM)],
        out_specs=pl.BlockSpec(memory_space=pltpu.SMEM),
        out_shape=jax.ShapeDtypeStruct((2,), jnp.int32),
        compiler_params=pltpu.CompilerParams(vmem_limit_bytes=VMEM_BYTES),
        name="gate",
    )(position)


def shift(array, by):
    return lax.ppermute(array, "x", [(i, (i + by) % 4) for i in range(4)])


def to_heads(packed):
    parts = [packed[0]]
    for s in (1, 2, 3):
        parts.append(lax.ppermute(packed[s], "zl", [(i, i ^ s) for i in range(4)]))
    return jnp.stack(parts)


def neighbours(block):
    left = shift(block, 1)
    right = shift(block, -1)
    return [left, right]


def forwarded(near0, near1):
    half = near0[0].shape[0] // 2
    far_a = shift(jnp.concatenate([near0[0][:half], near1[0][:half]]), 1)
    far_b = shift(jnp.concatenate([near0[1][half:], near1[1][half:]]), -1)
    return [far_a, far_b]


def attention(queries, keys, values):
    rows = queries.shape[0]
    position = jnp.stack([lax.axis_index("zl"), lax.axis_index("c")]).astype(jnp.int32)
    run = (2, PIECE, HEAD_DIM)
    c0 = pack(partial(pack_kv_kernel, 0), position, (keys, values), (run,))
    c1 = pack(partial(pack_kv_kernel, PIECE), position, (keys, values), (run,))
    q_packed = pack(pack_q_kernel, position, (queries,), ((rows, HEAD_DIM),))
    own0 = to_heads(c0)
    own1 = to_heads(c1)
    q_all = to_heads(q_packed)
    near0 = neighbours(own0)
    near1 = neighbours(own1)
    far = forwarded(near0, near1)
    state = None
    at = gate(position)
    for name, blocks in (("1", [own0, *near0]), ("2", [own1, *near1]), ("3", far)):
        state = flash(at, q_all, blocks, state, name == "3")
    return to_tokens(state, rows // 16)


def to_tokens(attended, strip):
    blocks = attended.reshape(32, 2 * strip, HEAD_DIM)
    blocks = lax.all_to_all(blocks, ("zl", "y", "zh"), 0, 0, tiled=True)
    blocks = blocks.reshape(32, 2, strip, HEAD_DIM)
    own = blocks[:, 0]
    other = lax.ppermute(blocks[:, 1], "c", [(0, 1), (1, 0)])
    first = lax.axis_index("c") == 0
    both = jnp.stack([jnp.where(first, own, other), jnp.where(first, other, own)], axis=1)
    out = both.reshape(2, 2, 16, strip, HEAD_DIM).transpose(3, 0, 2, 1, 4)
    return out.reshape(strip, 2, 32 * HEAD_DIM)


def solution(mesh):
    grid = Mesh(mesh.devices.reshape(4, 4, 4, 2, 2), ("zl", "x", "y", "zh", "c"))
    spec = P(("zl", "x"), None, ("y", "zh", "c"))
    return jax.shard_map(
        attention,
        mesh=grid,
        in_specs=(spec, spec, spec),
        out_specs=P(("zl", "x", "y", "zh", "c"), None, None),
        check_vma=False,
    )
```
